32 devices in a mesh: grp: 2 (over y), row: 16 (over z, x, core).
Axes of the slice: x: 2, y: 2, z: 4, core: 2. Of those that a mesh axis runs over, the one named last changes fastest.
Arguments:
- diag_blocks: float32 [8192, 512], P('row'), may hold values from -0.6 to 2.6
- lower_coupling: float32 [8192, 64], P('row'), may hold values from -0.3125 to 0.3125
- upper_coupling: float32 [8192, 64], P('row'), may hold values from -0.3125 to 0.3125
- right_sides: float32 [8192, 1024], P('row', 'grp'), parts along dimension 1, may hold values from -108 to 108
Outputs:
- solution: float32 [8192, 1024], P('row', 'grp'), parts along dimension 1
- res_norms: float32 [8, 1024], P(None, 'grp'), parts along dimension 1
The draws below stay inside these ranges and needn't reach their ends.
There are 2 independent parts, one for each index of `grp`. The reference program is written for one: setup_inputs(seed, part) draws one part's arguments, and reference() takes and returns one part's arrays. A program takes and returns all parts, laid end to end along the dimension named above; an argument that names none is the same for every part. Nothing has to cross between parts.
All inputs are finite; a program needn't handle non-finite values.
Results may differ from the reference program's by a relative error of at most 0.0001.
Values sent between devices are 32-bit elements; how exact they have to be, the bound alone decides.
No kernel may reach another device: no remote copies, remote signals or barrier semaphores. Data moves between devices by JAX's collectives and lax.ppermute only.
A program may use at most 64 MiB of HBM per device.

```python
import math
import jax
import jax.numpy as jnp
from jax import lax

B = 512
W = 64
C = 512
SWEEPS = 8
N = 8192
N_ROW = 16


def draw_diag_blocks(key, part):
    first, second = jax.random.split(jax.random.fold_in(key, 31), 2)
    noise = jnp.clip(jax.random.normal(first, (N, B), jnp.float32), -4.0, 4.0)
    noise = noise * (0.8 / math.sqrt(B))
    pivots = jax.random.uniform(second, (N, 1), jnp.float32, 1.0, 2.0)
    local_rows = (jnp.arange(N, dtype=jnp.int32) % B)[:, None]
    columns = jnp.arange(B, dtype=jnp.int32)[None, :]
    marker = (local_rows == columns).astype(jnp.float32)
    return (noise + marker * pivots).astype(jnp.float32)


def draw_right_sides(key, part):
    first, second, third = jax.random.split(jax.random.fold_in(key, 47), 3)
    base = jnp.clip(jax.random.normal(first, (N, C), jnp.float32), -4.0, 4.0)
    trend = jnp.exp(math.log(3.0) * jnp.arange(N, dtype=jnp.float32) / N)[:, None]
    row_scale = jnp.exp(jax.random.uniform(second, (N, 1), jnp.float32, math.log(0.3), math.log(3.0)))
    col_scale = jnp.exp(jax.random.uniform(third, (1, C), jnp.float32, math.log(0.3), math.log(3.0)))
    return (base * trend * row_scale * col_scale).astype(jnp.float32)


def block_levels(key, shape, shards, least, largest):
    gain = 1.0
    for position, parts in shards:
        draws = jax.random.uniform(jax.random.fold_in(jax.random.fold_in(key, 6), position), (parts,), jnp.float32, least / len(shards), largest / len(shards))
        gain = gain * jnp.repeat(jnp.exp(draws), shape[position] // parts).reshape((-1,) + (1,) * (len(shape) - 1 - position))
    return gain


def bell_draw(rng, extent, spread, most, shards=(), held_as=jnp.bfloat16):
    drawn = jax.random.normal(rng, extent, jnp.float32) * spread
    if len(shards) > 0:
        drawn = block_levels(rng, extent, shards, -0.22, 0.18) * drawn
    return jnp.clip(drawn, min=-most, max=most).astype(held_as)


def setup_inputs(seed: int = 0, part: int = 0) -> dict:
    seeds = jax.random.split(jax.random.key(seed), 5)
    part_keys = jax.random.split(jax.random.fold_in(seeds[4], part), 5)
    diag_blocks = draw_diag_blocks(jax.random.fold_in(seeds[4], 71), part)
    lower_coupling = bell_draw(seeds[1], (N, W), (6 * W) ** -0.5, 0.3125, ((0, 16),), jnp.float32)
    upper_coupling = bell_draw(seeds[2], (N, W), (6 * W) ** -0.5, 0.3125, ((0, 16),), jnp.float32)
    right_sides = draw_right_sides(jax.random.fold_in(jax.random.fold_in(seeds[4], part), 71), part)
    return dict(diag_blocks=diag_blocks, lower_coupling=lower_coupling, upper_coupling=upper_coupling, right_sides=right_sides)


def reference(diag_blocks, lower_coupling, upper_coupling, right_sides):
    blocks = diag_blocks.reshape(N_ROW, B, B)
    lower_blocks = lower_coupling.reshape(N_ROW, B, W)
    upper_blocks = upper_coupling.reshape(N_ROW, B, W)
    sources = right_sides.reshape(N_ROW, B, C)
    pivots = jnp.diagonal(blocks, axis1=1, axis2=2)[:, :, None]
    solution = jnp.zeros((N_ROW, B, C), jnp.float32)
    norm_list = []
    for sweep_index in range(SWEEPS):
        before_rims = jnp.concatenate([jnp.zeros((1, W, C), jnp.float32), solution[:-1, B - W:]], 0)
        after_rims = jnp.concatenate([solution[1:, :W], jnp.zeros((1, W, C), jnp.float32)], 0)
        images = jnp.einsum('kij,kjc->kic', blocks, solution, precision=lax.Precision.HIGHEST)
        images = images + jnp.einsum('kiw,kwc->kic', lower_blocks, before_rims, precision=lax.Precision.HIGHEST)
        images = images + jnp.einsum('kiw,kwc->kic', upper_blocks, after_rims, precision=lax.Precision.HIGHEST)
        residual = sources - images
        norm_list.append(jnp.sqrt(lax.optimization_barrier(jnp.sum(residual * residual, axis=(0, 1)))))
        solution = solution + residual / pivots
    return (solution.reshape(N_ROW * B, C), jnp.stack(norm_list))
```

```python
import functools

import jax
import jax.numpy as jnp
from jax import lax
from jax.experimental import pallas as pl
from jax.experimental.pallas import tpu as pltpu
from jax.sharding import PartitionSpec as P

SWEEPS = 8
F32 = jnp.float32
BF16 = jnp.bfloat16
VMEM_GRANT = 24 * 2**20
VMEM_BLOCK = pl.BlockSpec(memory_space=pltpu.VMEM)


def call(kernel, outs, *args, hbm=(), flops=0):
    args = [a if i in hbm else pltpu.with_memory_space_constraint(a, pltpu.VMEM) for i, a in enumerate(args)]
    many = isinstance(outs, (list, tuple))
    return pl.pallas_call(
        kernel,
        out_shape=outs,
        in_specs=[VMEM_BLOCK] * len(args),
        out_specs=[VMEM_BLOCK] * len(outs) if many else VMEM_BLOCK,
        compiler_params=pltpu.CompilerParams(vmem_limit_bytes=VMEM_GRANT),
        cost_estimate=pl.CostEstimate(flops=flops, transcendentals=0, bytes_accessed=0),
    )(*args)


def halves(x):
    high = x.astype(BF16)
    return high, (x - high.astype(F32)).astype(BF16)


def left_terms(x):
    high, low = halves(x)
    return jnp.concatenate([high, low, high], axis=1)


def right_terms(x):
    high, low = halves(x)
    return jnp.concatenate([high, high, low], axis=0)


def product(left, right):
    return jnp.dot(left, right, preferred_element_type=F32)


def place():
    index, size = lax.axis_index("row"), lax.axis_size("row")
    return index % 2, jnp.logical_or(index == 0, index == size - 1)


def rims(rows, width):
    odd, _ = place()
    top = rows - width
    return pl.multiple_of(odd * top, width), pl.multiple_of((1 - odd) * top, width)


def diagonal(block, offset):
    row = lax.broadcasted_iota(jnp.int32, block.shape, 0) + offset
    column = lax.broadcasted_iota(jnp.int32, block.shape, 1)
    return jnp.sum(jnp.where(row == column, block, 0.0), axis=1, keepdims=True)


def facing(outer):
    _, end = place()
    return jnp.where(end, jnp.zeros_like(outer), outer)


def opening(diag, sides, width):
    odd, _ = place()
    top = diag.shape[0] - width
    first = sides[:width] / diagonal(diag[:width, :width], 0)
    last = sides[top:] / diagonal(diag[top:, top:], 0)
    return facing(jnp.where(odd == 1, last, first)), jnp.where(odd == 1, first, last)


def setup_kernel(diag, lower, upper, sides, diag_out, coupling_out, pivot_out, x_out, v_out, sums_out):
    odd, _ = place()
    block, side = diag[...], sides[...]
    pivots = diagonal(block, 0)
    pivot_out[...] = jnp.broadcast_to(pivots, pivot_out.shape)
    x = side / pivots
    x_out[...] = x
    sums_out[0:1, :] = jnp.sum(side * side, axis=0, keepdims=True)
    low, up = lower[...], upper[...]
    outer = jnp.where(odd == 1, up, low)
    inner = jnp.where(odd == 1, low, up)
    coupling_out[...] = left_terms(jnp.concatenate([outer, inner], axis=1))
    left = left_terms(block)
    diag_out[...] = left
    v_out[...] = side - product(left, right_terms(x))


def halo_terms(outer, inner):
    return right_terms(jnp.concatenate([outer[...], inner[...]], axis=0))


def wide(pivots, columns):
    return jnp.concatenate([pivots] * (columns // pivots.shape[1]), axis=1)


def rim_kernel(outer, inner, x, v, coupling, pivots, outer_out, inner_out, *, width):
    rows, columns = x.shape
    far, near = rims(rows, width)
    pick = lambda ref: jnp.concatenate([ref[pl.ds(far, width), :], ref[pl.ds(near, width), :]], axis=0)
    residual = pick(v) - product(pick(coupling), halo_terms(outer, inner))
    new = pick(x) + residual / wide(pick(pivots), columns)
    outer_out[...] = facing(new[:width])
    inner_out[...] = new[width:]


def sweep_kernel(outer, inner, x, v, side, diag, coupling, pivots, sums, x_out, v_out, sums_out, *, sweep):
    columns = x.shape[1]
    sums_out[...] = sums[...]
    residual = v[...] - product(coupling[...], halo_terms(outer, inner))
    sums_out[sweep : sweep + 1, :] = jnp.sum(residual * residual, axis=0, keepdims=True)
    new = x[...] + residual / wide(pivots[...], columns)
    x_out[...] = new
    v_out[...] = side[...] - product(diag[...], right_terms(new))


def last_kernel(outer, inner, v, coupling, sums, r_out, sums_out, *, sweep):
    sums_out[...] = sums[...]
    residual = v[...] - product(coupling[...], halo_terms(outer, inner))
    sums_out[sweep : sweep + 1, :] = jnp.sum(residual * residual, axis=0, keepdims=True)
    r_out[...] = residual


def close_kernel(r, x, pivots, x_out):
    x_out[...] = x[...] + r[...] / wide(pivots[...], x.shape[1])


def pairings():
    size, groups = lax.axis_size("row"), lax.axis_size("grp")
    within = [(i, i ^ 1) for i in range(size)]
    between = []
    for g in range(groups):
        for i in range(size):
            j = i + 1 if i % 2 else i - 1
            if 0 <= j < size:
                target = g * size + j
            elif groups % 2 == 0:
                target = (g ^ 1) * size + i
            else:
                target = g * size + size - 1 - i
            between.append((g * size + i, target))
    return within, between


def exchange(outer, inner):
    within, between = pairings()
    return lax.ppermute(outer, ("grp", "row"), between), lax.ppermute(inner, "row", within)


def row_sum(x):
    size = lax.axis_size("row")
    assert size & (size - 1) == 0
    step = 1
    while step < size:
        flip = step if step == 1 else step + 1
        x = x + lax.ppermute(x, "row", [(i, i ^ flip) for i in range(size)])
        step *= 2
    return x


def local(diag_blocks, lower_coupling, upper_coupling, right_sides):
    rows, columns = right_sides.shape
    width = lower_coupling.shape[1]
    rim = pltpu.VMEM((width, columns), F32)
    panel = pltpu.VMEM((rows, columns), F32)
    sums_shape = pltpu.VMEM((SWEEPS, columns), F32)
    lanes = 128
    outer, inner = opening(diag_blocks, right_sides, width)
    outer, inner = exchange(outer, inner)
    diag, coupling, pivots, x, v, sums = call(
        setup_kernel,
        [
            pltpu.VMEM((rows, 3 * rows), BF16),
            pltpu.VMEM((rows, 6 * width), BF16),
            pltpu.VMEM((rows, lanes), F32),
            panel,
            panel,
            sums_shape,
        ],
        diag_blocks, lower_coupling, upper_coupling, right_sides,
        hbm=(0, 1, 2, 3),
        flops=6 * rows * rows * columns,
    )
    for sweep in range(1, SWEEPS - 1):
        sent = call(
            functools.partial(rim_kernel, width=width),
            [rim, rim],
            outer, inner, x, v, coupling, pivots,
            flops=24 * width * width * columns,
        )
        x, v, sums = call(
            functools.partial(sweep_kernel, sweep=sweep),
            [panel, panel, sums_shape],
            outer, inner, x, v, right_sides, diag, coupling, pivots, sums,
            hbm=(4,),
            flops=6 * rows * (rows + 2 * width) * columns,
        )
        outer, inner = exchange(*sent)
    r, sums = call(
        functools.partial(last_kernel, sweep=SWEEPS - 1),
        [panel, sums_shape],
        outer, inner, v, coupling, sums,
        flops=12 * rows * width * columns,
    )
    solution = call(close_kernel, jax.ShapeDtypeStruct((rows, columns), F32), r, x, pivots, flops=10 * rows * columns)
    return solution, jnp.sqrt(row_sum(sums))


def solution(mesh):
    return jax.shard_map(
        local,
        mesh=mesh,
        in_specs=(P("row", None), P("row", None), P("row", None), P("row", "grp")),
        out_specs=(P("row", "grp"), P(None, "grp")),
        check_vma=False,
    )
```

```python
import functools

import jax
import jax.numpy as jnp
from jax import lax
from jax.experimental import pallas as pl
from jax.experimental.pallas import tpu as pltpu
from jax.sharding import PartitionSpec as P


SWEEPS = 8
F32 = jnp.float32
BF16 = jnp.bfloat16
VMEM_GRANT = 24 * 2**20
HBM_BLOCK = pl.BlockSpec(memory_space=pltpu.HBM)
VMEM_BLOCK = pl.BlockSpec(memory_space=pltpu.VMEM)


def call(kernel, outs, *args, hbm=(), scratch=(), flops=0):
    args = [pltpu.with_memory_space_constraint(a, pltpu.HBM if i in hbm else pltpu.VMEM) for i, a in enumerate(args)]
    many = isinstance(outs, list)
    return pl.pallas_call(
        kernel,
        out_shape=outs,
        in_specs=[HBM_BLOCK if i in hbm else VMEM_BLOCK for i in range(len(args))],
        out_specs=[VMEM_BLOCK] * len(outs) if many else VMEM_BLOCK,
        scratch_shapes=scratch,
        compiler_params=pltpu.CompilerParams(vmem_limit_bytes=VMEM_GRANT),
        cost_estimate=pl.CostEstimate(flops=flops, transcendentals=0, bytes_accessed=0),
    )(*args)


def halves(x):
    high = x.astype(BF16)
    return high, (x - high.astype(F32)).astype(BF16)


def left_terms(x):
    high, low = halves(x)
    return jnp.concatenate([high, low, high], axis=1)


def right_terms(x):
    high, low = halves(x)
    return jnp.concatenate([high, high, low], axis=0)


def product(left, right):
    return jnp.dot(left, right, preferred_element_type=F32)


def place():
    index, size = lax.axis_index("row"), lax.axis_size("row")
    return index % 2, jnp.logical_or(index == 0, index == size - 1)


def rims(rows, width):
    odd, _ = place()
    top = rows - width
    return pl.multiple_of(odd * top, width), pl.multiple_of((1 - odd) * top, width)


def diagonal(block, offset):
    row = lax.broadcasted_iota(jnp.int32, block.shape, 0) + offset
    column = lax.broadcasted_iota(jnp.int32, block.shape, 1)
    return jnp.sum(jnp.where(row == column, block, 0.0), axis=1, keepdims=True)


def facing(outer):
    _, end = place()
    return jnp.where(end, jnp.zeros_like(outer), outer)


def copies(pairs, sems):
    moves = [pltpu.make_async_copy(source, target, sems.at[i]) for i, (source, target) in enumerate(pairs)]
    for move in moves:
        move.start()
    return moves


def open_kernel(diag, lower, upper, sides, outer_out, inner_out, corners, strips, low, up, sems):
    odd, end = place()
    rows, columns = sides.shape
    width, lanes = corners.shape[1:]
    top = rows - width
    moves = copies(
        [
            (diag.at[pl.ds(0, width), pl.ds(0, lanes)], corners.at[0]),
            (diag.at[pl.ds(top, width), pl.ds(rows - lanes, lanes)], corners.at[1]),
            (sides.at[pl.ds(0, width)], strips.at[0]),
            (sides.at[pl.ds(top, width)], strips.at[1]),
            (lower.at[:, pl.ds(0, lanes)], low),
            (upper.at[:, pl.ds(rows - lanes, lanes)], up),
        ],
        sems,
    )
    for move in moves:
        move.wait()
    head, tail = diagonal(corners[0], 0), diagonal(corners[1], lanes - width)
    first = strips[0] / head
    last = strips[1] / tail
    outer_out[:, :columns] = facing(jnp.where(odd == 1, last, first))
    coupling = facing(jnp.where(odd == 1, up[...].T[lanes - width :], low[...].T[:width]))
    pivots = jnp.where(end, 1.0, jnp.where(odd == 1, tail, head))
    outer_out[:, columns:] = jnp.concatenate([coupling, jnp.broadcast_to(pivots, coupling.shape)], axis=1)
    inner_out[...] = jnp.where(odd == 1, first, last)


def setup_kernel(diag, lower, upper, sides, diag_out, coupling_out, near_out, pivot_out, side_out, x_out, v_out, sums_out, block, low, up, sems):
    odd, _ = place()
    width, rows = low.shape
    moves = copies([(sides, side_out), (diag, block), (lower, low), (upper, up)], sems)
    moves[0].wait()
    side = side_out[...]
    sums_out[0:1, :] = jnp.sum(side * side, axis=0, keepdims=True)
    moves[1].wait()
    pivots = diagonal(block[...], 0)
    pivot_out[...] = jnp.broadcast_to(pivots, pivot_out.shape)
    x = side / pivots
    x_out[...] = x
    left = left_terms(block[...])
    diag_out[...] = left
    v_out[...] = side - product(left, right_terms(x))
    moves[2].wait()
    moves[3].wait()
    outer = jnp.where(odd == 1, up[...], low[...])
    inner = jnp.where(odd == 1, low[...], up[...])
    coupling = jnp.concatenate([outer, inner], axis=0).T
    coupling_out[...] = left_terms(coupling)
    top = rows - width
    inner = coupling[:, width:]
    near_out[...] = left_terms(jnp.where(odd == 1, inner[top:, :], inner[:width, :]))


def wide(pivots, columns):
    return jnp.concatenate([pivots] * (columns // pivots.shape[1]), axis=1)


def send_kernel(inner, x, v, near, pivots, outer_out):
    rows, columns = x.shape
    width = inner.shape[0]
    far, _ = rims(rows, width)
    pick = lambda ref: ref[pl.ds(far, width), :]
    residual = pick(v) - product(near[...], right_terms(inner[...]))
    outer_out[...] = facing(pick(x) + residual / wide(pick(pivots), columns))


def outer_halo(message, opened, mine):
    if mine is None:
        return message[:, : opened.shape[1] - 128]
    columns = message.shape[1]
    width = message.shape[0]
    extra = opened[:, columns:]
    term = product(left_terms(extra[:, :width]), right_terms(mine[...]))
    return message[...] - term / extra[:, width : width + 1]


def halo_terms(message, opened, mine, inner):
    return right_terms(jnp.concatenate([outer_halo(message, opened, mine), inner[...]], axis=0))


def keep_kernel(x, outer_out):
    far, _ = rims(x.shape[0], outer_out.shape[0])
    outer_out[...] = x[pl.ds(far, outer_out.shape[0]), :]


def rim_kernel(*refs, first):
    refs = list(refs)
    mine = None if first else refs.pop(0)
    message, opened, inner, x, v, coupling, pivots, inner_out = refs
    rows, columns = x.shape
    width = inner.shape[0]
    _, near = rims(rows, width)
    pick = lambda ref: ref[pl.ds(near, width), :]
    residual = pick(v) - product(pick(coupling), halo_terms(message, opened, mine, inner))
    inner_out[...] = pick(x) + residual / wide(pick(pivots), columns)


def sweep_kernel(*refs, sweep, first):
    refs = list(refs)
    mine = None if first else refs.pop(0)
    message, opened, inner, x, v, side, diag, coupling, pivots, sums, x_out, v_out, sums_out = refs
    _, columns = x.shape
    sums_out[...] = sums[...]
    residual = v[...] - product(coupling[...], halo_terms(message, opened, mine, inner))
    sums_out[sweep : sweep + 1, :] = jnp.sum(residual * residual, axis=0, keepdims=True)
    new = x[...] + residual / wide(pivots[...], columns)
    x_out[...] = new
    v_out[...] = side[...] - product(diag[...], right_terms(new))


def last_kernel(mine, message, opened, inner, v, coupling, sums, r_out, sums_out, *, sweep):
    sums_out[...] = sums[...]
    residual = v[...] - product(coupling[...], halo_terms(message, opened, mine, inner))
    sums_out[sweep : sweep + 1, :] = jnp.sum(residual * residual, axis=0, keepdims=True)
    r_out[...] = residual


def close_kernel(r, x, pivots, x_out):
    x_out[...] = x[...] + r[...] / wide(pivots[...], x.shape[1])


def pairings():
    size, groups = lax.axis_size("row"), lax.axis_size("grp")
    within = [(i, i ^ 1) for i in range(size)]
    between = []
    for g in range(groups):
        for i in range(size):
            j = i + 1 if i % 2 else i - 1
            if 0 <= j < size:
                target = g * size + j
            elif groups % 2 == 0:
                target = (g ^ 1) * size + i
            else:
                target = g * size + size - 1 - i
            between.append((g * size + i, target))
    return within, between


def across(outer):
    return lax.ppermute(outer, ("grp", "row"), pairings()[1])


def along(inner):
    return lax.ppermute(inner, "row", pairings()[0])


def row_sum(x):
    size = lax.axis_size("row")
    assert size & (size - 1) == 0
    step = 1
    while step < size:
        flip = step if step == 1 else step + 1
        x = x + lax.ppermute(x, "row", [(i, i ^ flip) for i in range(size)])
        step *= 2
    return x


def program(diag_blocks, lower_coupling, upper_coupling, right_sides):
    rows, columns = right_sides.shape
    width = lower_coupling.shape[1]
    rim = pltpu.VMEM((width, columns), F32)
    panel = pltpu.VMEM((rows, columns), F32)
    sums_shape = pltpu.VMEM((SWEEPS, columns), F32)
    lanes = 128
    lower, upper = lower_coupling.T, upper_coupling.T
    opened, inner = call(
        open_kernel,
        [pltpu.VMEM((width, columns + 2 * width), F32), rim],
        diag_blocks, lower, upper, right_sides,
        hbm=(0, 1, 2, 3),
        scratch=[
            pltpu.VMEM((2, width, lanes), F32),
            pltpu.VMEM((2, width, columns), F32),
            pltpu.VMEM((width, lanes), F32),
            pltpu.VMEM((width, lanes), F32),
            pltpu.SemaphoreType.DMA((6,)),
        ],
    )
    opened = message = across(opened)
    inner = along(inner)
    diag, coupling, near, pivots, side, x, v, sums = call(
        setup_kernel,
        [
            pltpu.VMEM((rows, 3 * rows), BF16),
            pltpu.VMEM((rows, 6 * width), BF16),
            pltpu.VMEM((width, 3 * width), BF16),
            pltpu.VMEM((rows, lanes), F32),
            panel,
            panel,
            panel,
            sums_shape,
        ],
        diag_blocks, lower, upper, right_sides,
        hbm=(0, 1, 2, 3),
        scratch=[
            pltpu.VMEM((rows, rows), F32),
            pltpu.VMEM((width, rows), F32),
            pltpu.VMEM((width, rows), F32),
            pltpu.SemaphoreType.DMA((4,)),
        ],
        flops=6 * rows * rows * columns,
    )
    mine = []
    for sweep in range(1, SWEEPS - 1):
        sent = call(send_kernel, rim, inner, x, v, near, pivots, flops=6 * width * width * columns)
        ahead = across(sent)
        kept = call(keep_kernel, rim, x)
        rim_values = call(
            functools.partial(rim_kernel, first=sweep == 1),
            rim,
            *mine, message, opened, inner, x, v, coupling, pivots,
            flops=18 * width * width * columns,
        )
        x, v, sums = call(
            functools.partial(sweep_kernel, sweep=sweep, first=sweep == 1),
            [panel, panel, sums_shape],
            *mine, message, opened, inner, x, v, side, diag, coupling, pivots, sums,
            flops=6 * rows * (rows + 2 * width) * columns,
        )
        mine, message, inner = [kept], ahead, along(rim_values)
    r, sums = call(
        functools.partial(last_kernel, sweep=SWEEPS - 1),
        [panel, sums_shape],
        *mine, message, opened, inner, v, coupling, sums,
        flops=12 * rows * width * columns,
    )
    solution = call(close_kernel, jax.ShapeDtypeStruct((rows, columns), F32), r, x, pivots, flops=10 * rows * columns)
    return solution, jnp.sqrt(row_sum(sums))


def solution(mesh):
    return jax.shard_map(
        program,
        mesh=mesh,
        in_specs=(P("row", None), P("row", None), P("row", None), P("row", "grp")),
        out_specs=(P("row", "grp"), P(None, "grp")),
        check_vma=False,
    )
```

```python
import functools

import jax
import jax.numpy as jnp
from jax import lax
from jax.experimental import pallas as pl
from jax.experimental.pallas import tpu as pltpu
from jax.sharding import PartitionSpec as P


SWEEPS = 8
F32 = jnp.float32
BF16 = jnp.bfloat16
VMEM_GRANT = 24 * 2**20
HBM_BLOCK = pl.BlockSpec(memory_space=pltpu.HBM)
VMEM_BLOCK = pl.BlockSpec(memory_space=pltpu.VMEM)


def call(kernel, outs, *args, hbm=(), scratch=(), flops=0):
    args = [pltpu.with_memory_space_constraint(a, pltpu.HBM if i in hbm else pltpu.VMEM) for i, a in enumerate(args)]
    many = isinstance(outs, list)
    return pl.pallas_call(
        kernel,
        out_shape=outs,
        in_specs=[HBM_BLOCK if i in hbm else VMEM_BLOCK for i in range(len(args))],
        out_specs=[VMEM_BLOCK] * len(outs) if many else VMEM_BLOCK,
        scratch_shapes=scratch,
        compiler_params=pltpu.CompilerParams(vmem_limit_bytes=VMEM_GRANT),
        cost_estimate=pl.CostEstimate(flops=flops, transcendentals=0, bytes_accessed=0),
    )(*args)


def halves(x):
    high = x.astype(BF16)
    return high, (x - high.astype(F32)).astype(BF16)


def left_terms(x):
    high, low = halves(x)
    return jnp.concatenate([high, low, high], axis=1)


def right_terms(x):
    high, low = halves(x)
    return jnp.concatenate([high, high, low], axis=0)


def product(left, right):
    return jnp.dot(left, right, preferred_element_type=F32)


def place():
    index, size = lax.axis_index("row"), lax.axis_size("row")
    return index % 2, jnp.logical_or(index == 0, index == size - 1)


def rims(rows, width):
    odd, _ = place()
    top = rows - width
    return pl.multiple_of(odd * top, width), pl.multiple_of((1 - odd) * top, width)


def diagonal(block, offset):
    row = lax.broadcasted_iota(jnp.int32, block.shape, 0) + offset
    column = lax.broadcasted_iota(jnp.int32, block.shape, 1)
    return jnp.sum(jnp.where(row == column, block, 0.0), axis=1, keepdims=True)


def facing(outer):
    _, end = place()
    return jnp.where(end, jnp.zeros_like(outer), outer)


def copies(pairs, sems):
    moves = [pltpu.make_async_copy(source, target, sems.at[i]) for i, (source, target) in enumerate(pairs)]
    for move in moves:
        move.start()
    return moves


def open_kernel(diag, lower, upper, sides, outer_out, inner_out, corners, strips, low, up, sems):
    odd, _ = place()
    rows, columns = sides.shape
    width, lanes = corners.shape[1:]
    top = rows - width
    moves = copies(
        [
            (diag.at[pl.ds(0, width), pl.ds(0, lanes)], corners.at[0]),
            (diag.at[pl.ds(top, width), pl.ds(rows - lanes, lanes)], corners.at[1]),
            (sides.at[pl.ds(0, width)], strips.at[0]),
            (sides.at[pl.ds(top, width)], strips.at[1]),
            (lower.at[:, pl.ds(0, lanes)], low),
            (upper.at[:, pl.ds(rows - lanes, lanes)], up),
        ],
        sems,
    )
    for move in moves:
        move.wait()
    head, tail = diagonal(corners[0], 0), diagonal(corners[1], lanes - width)
    first = strips[0] / head
    last = strips[1] / tail
    outer_out[:, :columns] = facing(jnp.where(odd == 1, last, first))
    coupling = jnp.where(odd == 1, up[...].T[lanes - width :] / tail, low[...].T[:width] / head)
    outer_out[:, columns:] = jnp.concatenate([facing(coupling), jnp.zeros_like(coupling)], axis=1)
    inner_out[...] = jnp.where(odd == 1, first, last)


def setup_kernel(diag, lower, upper, sides, diag_out, outer_out, inner_out, scale_out, side_out, x_out, terms_out, v_out, sums_out, block, low, up, sems):
    odd, _ = place()
    _, rows = low.shape
    moves = copies([(sides, side_out), (diag, block), (lower, low), (upper, up)], sems)
    moves[0].wait()
    side = side_out[...]
    sums_out[0:1, :] = jnp.sum(side * side, axis=0, keepdims=True)
    moves[1].wait()
    scale = 1.0 / diagonal(block[...], 0)
    scale_out[...] = jnp.broadcast_to(scale, scale_out.shape)
    x = side * scale
    x_out[...] = x
    terms_out[...] = right_terms(x)
    diag_out[...] = left_terms(block[...])
    far, _ = spans(rows)
    v_out[...] = applied(side_out, diag_out, terms_out, far)
    moves[2].wait()
    moves[3].wait()
    low, up = low[...], up[...]
    outer_out[...] = left_terms(jnp.where(odd == 1, up, low).T)
    inner_out[...] = left_terms(jnp.where(odd == 1, low, up).T)


def spans(rows):
    odd, _ = place()
    half = rows // 2
    return pl.multiple_of(odd * half, half), pl.multiple_of((1 - odd) * half, half)


def applied(side, diag, terms, start):
    some = pl.ds(start, side.shape[0] // 2)
    return side[some, :] - product(diag[some, :], terms[...])


def wide(pivots, columns):
    return jnp.concatenate([pivots] * (columns // pivots.shape[1]), axis=1)


def send_kernel(inner, x, v, coupling, scale, outer_out):
    odd, _ = place()
    rows, columns = x.shape
    width = inner.shape[0]
    far, _ = rims(rows, width)
    rim = pl.ds(far, width)
    inside = pl.ds(pl.multiple_of(odd * (v.shape[0] - width), width), width)
    residual = v[inside, :] - product(coupling[rim, :], right_terms(inner[...]))
    outer_out[...] = facing(x[rim, :] + residual * wide(scale[rim, :], columns))


def fill_kernel(inner, terms, v, side, diag, coupling, u_out):
    far, near = spans(side.shape[0])
    half = v.shape[0]
    halo = right_terms(inner[...])
    u_out[pl.ds(far, half), :] = v[...] - product(coupling[pl.ds(far, half), :], halo)
    u_out[pl.ds(near, half), :] = applied(side, diag, terms, near) - product(coupling[pl.ds(near, half), :], halo)


def outer_halo(message, correction):
    if correction is None:
        return message[:, : message.shape[1] - 128]
    return message[...] - correction[...]


def rim_kernel(*refs, first):
    refs = list(refs)
    correction = None if first else refs.pop(0)
    message, x, u, coupling, scale, halo_out, inner_out = refs
    rows, columns = x.shape
    width = inner_out.shape[0]
    _, near = rims(rows, width)
    rim = pl.ds(near, width)
    halo = right_terms(outer_halo(message, correction))
    halo_out[...] = halo
    residual = u[rim, :] - product(coupling[rim, :], halo)
    inner_out[...] = x[rim, :] + residual * wide(scale[rim, :], columns)


def sweep_kernel(halo, opened, x, terms, u, side, diag, coupling, scale, sums, x_out, terms_out, v_out, correction_out, sums_out, *, sweep):
    rows, columns = x.shape
    width = opened.shape[0]
    far, _ = rims(rows, width)
    mine = jnp.concatenate([terms[pl.ds(far + part * rows, width), :] for part in range(3)], axis=0)
    correction_out[...] = product(left_terms(opened[:, columns : columns + width]), mine)
    sums_out[...] = sums[...]
    residual = u[...] - product(coupling[...], halo[...])
    sums_out[sweep : sweep + 1, :] = jnp.sum(residual * residual, axis=0, keepdims=True)
    new = x[...] + residual * wide(scale[...], columns)
    x_out[...] = new
    terms_out[...] = right_terms(new)
    start, _ = spans(rows)
    v_out[...] = applied(side, diag, terms_out, start)


def last_kernel(correction, message, u, coupling, sums, r_out, sums_out, *, sweep):
    sums_out[...] = sums[...]
    residual = u[...] - product(coupling[...], right_terms(outer_halo(message, correction)))
    sums_out[sweep : sweep + 1, :] = jnp.sum(residual * residual, axis=0, keepdims=True)
    r_out[...] = residual


def close_kernel(r, x, scale, x_out):
    x_out[...] = x[...] + r[...] * wide(scale[...], x.shape[1])


def pairings():
    size, groups = lax.axis_size("row"), lax.axis_size("grp")
    within = [(i, i ^ 1) for i in range(size)]
    between = []
    for g in range(groups):
        for i in range(size):
            j = i + 1 if i % 2 else i - 1
            if 0 <= j < size:
                target = g * size + j
            elif groups % 2 == 0:
                target = (g ^ 1) * size + i
            else:
                target = g * size + size - 1 - i
            between.append((g * size + i, target))
    return within, between


def across(outer):
    return lax.ppermute(outer, ("grp", "row"), pairings()[1])


def along(inner):
    return lax.ppermute(inner, "row", pairings()[0])


def row_sum(x):
    size = lax.axis_size("row")
    assert size & (size - 1) == 0
    step = 1
    while step < size:
        flip = step if step == 1 else step + 1
        x = x + lax.ppermute(x, "row", [(i, i ^ flip) for i in range(size)])
        step *= 2
    return x


def program(diag_blocks, lower_coupling, upper_coupling, right_sides):
    rows, columns = right_sides.shape
    width = lower_coupling.shape[1]
    rim = pltpu.VMEM((width, columns), F32)
    panel = pltpu.VMEM((rows, columns), F32)
    sums_shape = pltpu.VMEM((SWEEPS, columns), F32)
    lanes = 128
    lower, upper = lower_coupling.T, upper_coupling.T
    opened, inner = call(
        open_kernel,
        [pltpu.VMEM((width, columns + 2 * width), F32), rim],
        diag_blocks, lower, upper, right_sides,
        hbm=(0, 1, 2, 3),
        scratch=[
            pltpu.VMEM((2, width, lanes), F32),
            pltpu.VMEM((2, width, columns), F32),
            pltpu.VMEM((width, lanes), F32),
            pltpu.VMEM((width, lanes), F32),
            pltpu.SemaphoreType.DMA((6,)),
        ],
    )
    opened = message = across(opened)
    inner = along(inner)
    half = pltpu.VMEM((rows // 2, columns), F32)
    all_terms = pltpu.VMEM((3 * rows, columns), BF16)
    coupling_shape = pltpu.VMEM((rows, 3 * width), BF16)
    diag, outward, inward, scale, side, x, terms, v, sums = call(
        setup_kernel,
        [
            pltpu.VMEM((rows, 3 * rows), BF16),
            coupling_shape,
            coupling_shape,
            pltpu.VMEM((rows, lanes), F32),
            panel,
            panel,
            all_terms,
            half,
            sums_shape,
        ],
        diag_blocks, lower, upper, right_sides,
        hbm=(0, 1, 2, 3),
        scratch=[
            pltpu.VMEM((rows, rows), F32),
            pltpu.VMEM((width, rows), F32),
            pltpu.VMEM((width, rows), F32),
            pltpu.SemaphoreType.DMA((4,)),
        ],
        flops=3 * rows * rows * columns,
    )
    correction = []
    for sweep in range(1, SWEEPS):
        if sweep < SWEEPS - 1:
            sent = call(send_kernel, rim, inner, x, v, inward, scale, flops=6 * width * width * columns)
            ahead = across(sent)
        u = call(
            fill_kernel,
            panel,
            inner, terms, v, side, diag, inward,
            flops=3 * rows * (rows + 2 * width) * columns,
        )
        if sweep == SWEEPS - 1:
            break
        halo, rim_values = call(
            functools.partial(rim_kernel, first=sweep == 1),
            [pltpu.VMEM((3 * width, columns), BF16), rim],
            *correction, message, x, u, outward, scale,
            flops=6 * width * width * columns,
        )
        inner = along(rim_values)
        x, terms, v, kept, sums = call(
            functools.partial(sweep_kernel, sweep=sweep),
            [panel, all_terms, half, rim, sums_shape],
            halo, opened, x, terms, u, side, diag, outward, scale, sums,
            flops=3 * rows * (rows + 2 * width) * columns,
        )
        correction, message = [kept], ahead
    r, sums = call(
        functools.partial(last_kernel, sweep=SWEEPS - 1),
        [panel, sums_shape],
        *correction, message, u, outward, sums,
        flops=6 * rows * width * columns,
    )
    solution = call(close_kernel, jax.ShapeDtypeStruct((rows, columns), F32), r, x, scale, flops=10 * rows * columns)
    return solution, jnp.sqrt(row_sum(sums))


def solution(mesh):
    return jax.shard_map(
        program,
        mesh=mesh,
        in_specs=(P("row", None), P("row", None), P("row", None), P("row", "grp")),
        out_specs=(P("row", "grp"), P(None, "grp")),
        check_vma=False,
    )
```

```python
import functools

import jax
import jax.numpy as jnp
from jax import lax
from jax.experimental import pallas as pl
from jax.experimental.pallas import tpu as pltpu
from jax.sharding import PartitionSpec as P


SWEEPS = 8
F32 = jnp.float32
BF16 = jnp.bfloat16
VMEM_GRANT = 24 * 2**20
HBM_BLOCK = pl.BlockSpec(memory_space=pltpu.HBM)
VMEM_BLOCK = pl.BlockSpec(memory_space=pltpu.VMEM)


def call(kernel, outs, *args, hbm=(), free=(), scratch=(), flops=0):
    args = [a if i in free else pltpu.with_memory_space_constraint(a, pltpu.HBM if i in hbm else pltpu.VMEM) for i, a in enumerate(args)]
    many = isinstance(outs, list)
    return pl.pallas_call(
        kernel,
        out_shape=outs,
        in_specs=[HBM_BLOCK if i in hbm else VMEM_BLOCK for i in range(len(args))],
        out_specs=[VMEM_BLOCK] * len(outs) if many else VMEM_BLOCK,
        scratch_shapes=scratch,
        compiler_params=pltpu.CompilerParams(vmem_limit_bytes=VMEM_GRANT),
        cost_estimate=pl.CostEstimate(flops=flops, transcendentals=0, bytes_accessed=0),
    )(*args)


def halves(x):
    high = x.astype(BF16)
    return high, (x - high.astype(F32)).astype(BF16)


def left_terms(x):
    high, low = halves(x)
    return jnp.concatenate([high, low, high], axis=1)


def right_terms(x):
    high, low = halves(x)
    return jnp.concatenate([high, high, low], axis=0)


def both(x, axis):
    return jnp.concatenate(halves(x), axis=axis)


def product(left, right):
    return jnp.dot(left, right, preferred_element_type=F32)


def place():
    index, size = lax.axis_index("row"), lax.axis_size("row")
    return index % 2, jnp.logical_or(index == 0, index == size - 1)


def rims(rows, width):
    odd, _ = place()
    top = rows - width
    return pl.multiple_of(odd * top, width), pl.multiple_of((1 - odd) * top, width)


def diagonal(block, offset):
    row = lax.broadcasted_iota(jnp.int32, block.shape, 0) + offset
    column = lax.broadcasted_iota(jnp.int32, block.shape, 1)
    return jnp.sum(jnp.where(row == column, block, 0.0), axis=1, keepdims=True)


def facing(outer):
    _, end = place()
    return jnp.where(end, jnp.zeros_like(outer), outer)


def copies(pairs, sems):
    moves = [pltpu.make_async_copy(source, target, sems.at[i]) for i, (source, target) in enumerate(pairs)]
    for move in moves:
        move.start()
    return moves


def open_kernel(diag, sides, lower, upper, outer_out, inner_out, corners, strips, sems):
    odd, _ = place()
    rows = sides.shape[0]
    width, lanes = corners.shape[1:]
    top = rows - width
    moves = copies(
        [
            (diag.at[pl.ds(0, width), pl.ds(0, lanes)], corners.at[0]),
            (diag.at[pl.ds(top, width), pl.ds(rows - lanes, lanes)], corners.at[1]),
            (sides.at[pl.ds(0, width)], strips.at[0]),
            (sides.at[pl.ds(top, width)], strips.at[1]),
        ],
        sems,
    )
    for move in moves:
        move.wait()
    first = strips[0] / diagonal(corners[0], 0)
    last = strips[1] / diagonal(corners[1], lanes - width)
    outer_out[...] = facing(jnp.where(odd == 1, last, first))
    inner_out[...] = jnp.where(odd == 1, first, last)


def setup_kernel(block, low, up, sides, diag_out, outer_out, inner_out, told_out, scale_out, x_out, terms_out, v_out, sums_out):
    odd, _ = place()
    width, rows = low.shape
    side = sides[...]
    sums_out[0:1, :] = jnp.sum(side * side, axis=0, keepdims=True)
    scale = 1.0 / diagonal(block[...], 0)
    scale_out[...] = jnp.broadcast_to(scale, scale_out.shape)
    x = side * scale
    x_out[...] = x
    terms_out[...] = both(x, 0)
    diag_out[...] = both(block[...], 1)
    far, _ = spans(rows)
    v_out[...] = applied(sides, diag_out, terms_out, far)
    low, up = low[...], up[...]
    outer = jnp.where(odd == 1, up, low).T
    outer_out[...] = left_terms(outer)
    told = jnp.where(odd == 1, outer[rows - width :], outer[:width])
    told = told * jnp.where(odd == 1, scale[rows - width :], scale[:width])
    told_out[...] = facing(packed(told))
    inner_out[...] = left_terms(jnp.where(odd == 1, low, up).T)


def packed(square):
    return jnp.concatenate([square[i : i + 8] for i in range(0, square.shape[0], 8)], axis=1)


def unpacked(strip, width):
    return jnp.concatenate([strip[:, i : i + width] for i in range(0, width * width // 8, width)], axis=0)


def spans(rows):
    odd, _ = place()
    half = rows // 2
    return pl.multiple_of(odd * half, half), pl.multiple_of((1 - odd) * half, half)


def applied(side, diag, terms, start):
    rows = side.shape[0]
    some = pl.ds(start, rows // 2)
    high, low = diag[some, :rows], diag[some, rows:]
    images = product(high, terms[rows:, :]) + product(low, terms[:rows, :]) + product(high, terms[:rows, :])
    return side[some, :] - images


def wide(pivots, columns):
    return jnp.concatenate([pivots] * (columns // pivots.shape[1]), axis=1)


def send_kernel(*refs):
    *told, inner, x, v, coupling, scale, outer_out = refs
    odd, _ = place()
    rows, columns = x.shape
    width = inner.shape[0]
    far, _ = rims(rows, width)
    rim = pl.ds(far, width)
    inside = pl.ds(pl.multiple_of(odd * (v.shape[0] - width), width), width)
    residual = v[inside, :] - product(coupling[rim, :], right_terms(inner[...]))
    outer_out[:width, :] = facing(x[rim, :] + residual * wide(scale[rim, :], columns))
    if told:
        outer_out[width:, :] = told[0][...]


def fill_kernel(inner, terms, v, side, diag, coupling, u_out):
    far, near = spans(side.shape[0])
    half = v.shape[0]
    halo = right_terms(inner[...])
    u_out[pl.ds(far, half), :] = v[...] - product(coupling[pl.ds(far, half), :], halo)
    u_out[pl.ds(near, half), :] = applied(side, diag, terms, near) - product(coupling[pl.ds(near, half), :], halo)


def rim_kernel(*refs, sweep):
    told_out = None
    if sweep == 2:
        *refs, told_out = refs
    *known, message, x, u, coupling, scale, halo_out, inner_out = refs
    rows, columns = x.shape
    width = inner_out.shape[0]
    _, near = rims(rows, width)
    rim = pl.ds(near, width)
    outer = message[:width, :]
    if sweep == 2:
        told = left_terms(unpacked(message[width:, :], width))
        told_out[...] = told
        outer = outer - product(told, known[0][...])
    elif sweep > 2:
        outer = outer - known[0][...]
    halo = right_terms(outer)
    halo_out[...] = halo
    residual = u[rim, :] - product(coupling[rim, :], halo)
    inner_out[...] = x[rim, :] + residual * wide(scale[rim, :], columns)


def sweep_kernel(*refs, sweep):
    *told, halo, x, terms, u, side, diag, coupling, scale, sums, x_out, terms_out, v_out, known_out, sums_out = refs
    rows, columns = x.shape
    width = halo.shape[0] // 3
    far, _ = rims(rows, width)
    mine = jnp.concatenate([terms[pl.ds(far + part * rows, width), :] for part in (0, 0, 1)], axis=0)
    known_out[...] = product(told[0][...], mine) if told else mine
    sums_out[...] = sums[...]
    residual = u[...] - product(coupling[...], halo[...])
    sums_out[sweep : sweep + 1, :] = jnp.sum(residual * residual, axis=0, keepdims=True)
    new = x[...] + residual * wide(scale[...], columns)
    x_out[...] = new
    terms_out[...] = both(new, 0)
    start, _ = spans(rows)
    v_out[...] = applied(side, diag, terms_out, start)


def last_kernel(known, message, u, coupling, sums, r_out, sums_out, *, sweep):
    sums_out[...] = sums[...]
    residual = u[...] - product(coupling[...], right_terms(message[...] - known[...]))
    sums_out[sweep : sweep + 1, :] = jnp.sum(residual * residual, axis=0, keepdims=True)
    r_out[...] = residual


def close_kernel(r, x, scale, x_out):
    x_out[...] = x[...] + r[...] * wide(scale[...], x.shape[1])


def pairings():
    size, groups = lax.axis_size("row"), lax.axis_size("grp")
    within = [(i, i ^ 1) for i in range(size)]
    between = []
    for g in range(groups):
        for i in range(size):
            j = i + 1 if i % 2 else i - 1
            if 0 <= j < size:
                target = g * size + j
            elif groups % 2 == 0:
                target = (g ^ 1) * size + i
            else:
                target = g * size + size - 1 - i
            between.append((g * size + i, target))
    return within, between


def across(outer):
    return lax.ppermute(outer, ("grp", "row"), pairings()[1])


def along(inner):
    return lax.ppermute(inner, "row", pairings()[0])


def row_sum(x):
    size = lax.axis_size("row")
    assert size & (size - 1) == 0
    step = 1
    while step < size:
        flips = [1] if step == 1 else [step + 1, 2 * step + 1, 3 * step] if 2 * step < size else [step + 1]
        x = functools.reduce(jnp.add, [x] + [lax.ppermute(x, "row", [(i, i ^ f) for i in range(size)]) for f in flips])
        step *= 1 + len(flips)
    return x


def program(diag_blocks, lower_coupling, upper_coupling, right_sides):
    rows, columns = right_sides.shape
    width = lower_coupling.shape[1]
    rim = pltpu.VMEM((width, columns), F32)
    panel = pltpu.VMEM((rows, columns), F32)
    sums_shape = pltpu.VMEM((SWEEPS, columns), F32)
    lanes = 128
    lower, upper = lower_coupling.T, upper_coupling.T
    outer, inner = call(
        open_kernel,
        [rim, rim],
        diag_blocks, right_sides, lower, upper,
        hbm=(0, 1, 2, 3),
        scratch=[
            pltpu.VMEM((2, width, lanes), F32),
            pltpu.VMEM((2, width, columns), F32),
            pltpu.SemaphoreType.DMA((4,)),
        ],
    )
    message = across(outer)
    inner = along(inner)
    half = pltpu.VMEM((rows // 2, columns), F32)
    all_terms = pltpu.VMEM((2 * rows, columns), BF16)
    coupling_shape = pltpu.VMEM((rows, 3 * width), BF16)
    diag, outward, inward, told, scale, x, terms, v, sums = call(
        setup_kernel,
        [
            pltpu.VMEM((rows, 2 * rows), BF16),
            coupling_shape,
            coupling_shape,
            pltpu.VMEM((8, width * width // 8), F32),
            pltpu.VMEM((rows, lanes), F32),
            panel,
            all_terms,
            half,
            sums_shape,
        ],
        diag_blocks, lower, upper, right_sides,
        free=(0, 1, 2, 3),
        flops=3 * rows * rows * columns,
    )
    known, heard = [], []
    halo_shape = pltpu.VMEM((3 * width, columns), BF16)
    for sweep in range(1, SWEEPS):
        if sweep < SWEEPS - 1:
            tell = [told] if sweep == 1 else []
            sent = call(
                send_kernel,
                pltpu.VMEM((width + 8 * len(tell), columns), F32),
                *tell, inner, x, v, inward, scale,
                flops=6 * width * width * columns,
            )
            ahead = across(sent)
        u = call(
            fill_kernel,
            panel,
            inner, terms, v, right_sides, diag, inward,
            free=(3,),
            flops=3 * rows * (rows + 2 * width) * columns,
        )
        if sweep == SWEEPS - 1:
            break
        halo, rim_values, *news = call(
            functools.partial(rim_kernel, sweep=sweep),
            [halo_shape, rim] + ([pltpu.VMEM((width, 3 * width), BF16)] if sweep == 2 else []),
            *known, message, x, u, outward, scale,
            flops=6 * width * width * columns,
        )
        inner = along(rim_values)
        heard = heard or news
        x, terms, v, kept, sums = call(
            functools.partial(sweep_kernel, sweep=sweep),
            [panel, all_terms, half, rim if heard else halo_shape, sums_shape],
            *heard, halo, x, terms, u, right_sides, diag, outward, scale, sums,
            free=(len(heard) + 4,),
            flops=3 * rows * (rows + 2 * width) * columns,
        )
        known, message = [kept], ahead
    r, sums = call(
        functools.partial(last_kernel, sweep=SWEEPS - 1),
        [panel, sums_shape],
        *known, message, u, outward, sums,
        flops=6 * rows * width * columns,
    )
    solution = call(close_kernel, jax.ShapeDtypeStruct((rows, columns), F32), r, x, scale, flops=10 * rows * columns)
    return solution, jnp.sqrt(row_sum(sums))


def solution(mesh):
    return jax.shard_map(
        program,
        mesh=mesh,
        in_specs=(P("row", None), P("row", None), P("row", None), P("row", "grp")),
        out_specs=(P("row", "grp"), P(None, "grp")),
        check_vma=False,
    )
```

```python
import functools

import jax
import jax.numpy as jnp
from jax import lax
from jax.experimental import pallas as pl
from jax.experimental.pallas import tpu as pltpu
from jax.sharding import PartitionSpec as P


SWEEPS = 8
F32 = jnp.float32
BF16 = jnp.bfloat16
VMEM_GRANT = 24 * 2**20
HBM_BLOCK = pl.BlockSpec(memory_space=pltpu.HBM)
VMEM_BLOCK = pl.BlockSpec(memory_space=pltpu.VMEM)


def call(kernel, outs, *args, hbm=(), free=(), scratch=(), flops=0):
    args = [a if i in free else pltpu.with_memory_space_constraint(a, pltpu.HBM if i in hbm else pltpu.VMEM) for i, a in enumerate(args)]
    many = isinstance(outs, list)
    return pl.pallas_call(
        kernel,
        out_shape=outs,
        in_specs=[HBM_BLOCK if i in hbm else VMEM_BLOCK for i in range(len(args))],
        out_specs=[VMEM_BLOCK] * len(outs) if many else VMEM_BLOCK,
        scratch_shapes=scratch,
        compiler_params=pltpu.CompilerParams(vmem_limit_bytes=VMEM_GRANT),
        cost_estimate=pl.CostEstimate(flops=flops, transcendentals=0, bytes_accessed=0),
    )(*args)


def halves(x):
    high = x.astype(BF16)
    return high, (x - high.astype(F32)).astype(BF16)


def left_terms(x):
    high, low = halves(x)
    return jnp.concatenate([high, low, high], axis=1)


def right_terms(x):
    high, low = halves(x)
    return jnp.concatenate([high, high, low], axis=0)


def both(x, axis):
    return jnp.concatenate(halves(x), axis=axis)


def product(left, right):
    return jnp.dot(left, right, preferred_element_type=F32)


def place():
    index, size = lax.axis_index("row"), lax.axis_size("row")
    return index % 2, jnp.logical_or(index == 0, index == size - 1)


def rims(rows, width):
    odd, _ = place()
    top = rows - width
    return pl.multiple_of(odd * top, width), pl.multiple_of((1 - odd) * top, width)


def diagonal(block, offset):
    row = lax.broadcasted_iota(jnp.int32, block.shape, 0) + offset
    column = lax.broadcasted_iota(jnp.int32, block.shape, 1)
    return jnp.sum(jnp.where(row == column, block, 0.0), axis=1, keepdims=True)


def facing(outer):
    _, end = place()
    return jnp.where(end, jnp.zeros_like(outer), outer)


def copies(pairs, sems):
    moves = [pltpu.make_async_copy(source, target, sems.at[i]) for i, (source, target) in enumerate(pairs)]
    for move in moves:
        move.start()
    return moves


def open_kernel(diag, sides, lower, upper, outer_out, corner, strip, sems):
    odd, _ = place()
    rows = sides.shape[0]
    width, lanes = corner.shape
    far, _ = rims(rows, width)
    tile = pl.ds(pl.multiple_of(odd * (rows - lanes), lanes), lanes)
    moves = copies([(diag.at[pl.ds(far, width), tile], corner), (sides.at[pl.ds(far, width)], strip)], sems)
    for move in moves:
        move.wait()
    outer_out[...] = facing(strip[...] / diagonal(corner[...], odd * (lanes - width)))


def inner_kernel(diag, sides, inner_out):
    odd, _ = place()
    rows = sides.shape[0]
    width, lanes = inner_out.shape[0], 128
    top = rows - width
    first = sides[:width, :] / diagonal(diag[:width, :lanes], 0)
    last = sides[top:, :] / diagonal(diag[top:, rows - lanes :], lanes - width)
    inner_out[...] = jnp.where(odd == 1, first, last)


def setup_kernel(block, low, up, sides, diag_out, outer_out, inner_out, told_out, scale_out, x_out, terms_out, v_out, sums_out):
    odd, _ = place()
    width, rows = low.shape
    side = sides[...]
    sums_out[0:1, :] = jnp.sum(side * side, axis=0, keepdims=True)
    scale = 1.0 / diagonal(block[...], 0)
    scale_out[...] = jnp.broadcast_to(scale, scale_out.shape)
    x = side * scale
    x_out[...] = x
    terms_out[...] = both(x, 0)
    diag_out[...] = both(block[...], 1)
    far, _ = spans(rows)
    v_out[...] = applied(sides, diag_out, terms_out, far)
    low, up = low[...], up[...]
    outer = jnp.where(odd == 1, up, low).T
    outer_out[...] = left_terms(outer)
    told = jnp.where(odd == 1, outer[rows - width :], outer[:width])
    told = told * jnp.where(odd == 1, scale[rows - width :], scale[:width])
    told_out[...] = facing(packed(told))
    inner_out[...] = left_terms(jnp.where(odd == 1, low, up).T)


def packed(square):
    return jnp.concatenate([square[i : i + 8] for i in range(0, square.shape[0], 8)], axis=1)


def unpacked(strip, width):
    return jnp.concatenate([strip[:, i : i + width] for i in range(0, width * width // 8, width)], axis=0)


def spans(rows):
    odd, _ = place()
    half = rows // 2
    return pl.multiple_of(odd * half, half), pl.multiple_of((1 - odd) * half, half)


def applied(side, diag, terms, start):
    rows = side.shape[0]
    some = pl.ds(start, rows // 2)
    high, low = diag[some, :rows], diag[some, rows:]
    images = product(high, terms[rows:, :]) + product(low, terms[:rows, :]) + product(high, terms[:rows, :])
    return side[some, :] - images


def wide(pivots, columns):
    return jnp.concatenate([pivots] * (columns // pivots.shape[1]), axis=1)


def send_kernel(*refs):
    *told, inner, x, v, coupling, scale, outer_out = refs
    odd, _ = place()
    rows, columns = x.shape
    width = inner.shape[0]
    far, _ = rims(rows, width)
    rim = pl.ds(far, width)
    inside = pl.ds(pl.multiple_of(odd * (v.shape[0] - width), width), width)
    residual = v[inside, :] - product(coupling[rim, :], right_terms(inner[...]))
    outer_out[:width, :] = facing(x[rim, :] + residual * wide(scale[rim, :], columns))
    if told:
        outer_out[width:, :] = told[0][...]


def fill_kernel(inner, terms, v, side, diag, coupling, u_out):
    far, near = spans(side.shape[0])
    half = v.shape[0]
    halo = right_terms(inner[...])
    u_out[pl.ds(far, half), :] = v[...] - product(coupling[pl.ds(far, half), :], halo)
    u_out[pl.ds(near, half), :] = applied(side, diag, terms, near) - product(coupling[pl.ds(near, half), :], halo)


def rim_kernel(*refs, sweep):
    told_out = None
    if sweep == 2:
        *refs, told_out = refs
    *known, message, x, u, coupling, scale, halo_out, inner_out = refs
    rows, columns = x.shape
    width = inner_out.shape[0]
    _, near = rims(rows, width)
    rim = pl.ds(near, width)
    outer = message[:width, :]
    if sweep == 2:
        told = left_terms(unpacked(message[width:, :], width))
        told_out[...] = told
        outer = outer - product(told, known[0][...])
    elif sweep > 2:
        outer = outer - known[0][...]
    halo = right_terms(outer)
    halo_out[...] = halo
    residual = u[rim, :] - product(coupling[rim, :], halo)
    inner_out[...] = x[rim, :] + residual * wide(scale[rim, :], columns)


def sweep_kernel(*refs, sweep):
    *told, halo, x, terms, u, side, diag, coupling, scale, sums, x_out, terms_out, v_out, known_out, sums_out = refs
    rows, columns = x.shape
    width = halo.shape[0] // 3
    far, _ = rims(rows, width)
    mine = jnp.concatenate([terms[pl.ds(far + part * rows, width), :] for part in (0, 0, 1)], axis=0)
    known_out[...] = product(told[0][...], mine) if told else mine
    sums_out[...] = sums[...]
    residual = u[...] - product(coupling[...], halo[...])
    sums_out[sweep : sweep + 1, :] = jnp.sum(residual * residual, axis=0, keepdims=True)
    new = x[...] + residual * wide(scale[...], columns)
    x_out[...] = new
    terms_out[...] = both(new, 0)
    start, _ = spans(rows)
    v_out[...] = applied(side, diag, terms_out, start)


def last_kernel(known, message, u, coupling, sums, halo_out, sums_out, *, sweep):
    sums_out[...] = sums[...]
    halo = right_terms(message[...] - known[...])
    halo_out[...] = halo
    residual = u[...] - product(coupling[...], halo)
    sums_out[sweep : sweep + 1, :] = jnp.sum(residual * residual, axis=0, keepdims=True)


def close_kernel(halo, u, coupling, x, scale, x_out):
    residual = u[...] - product(coupling[...], halo[...])
    x_out[...] = x[...] + residual * wide(scale[...], x.shape[1])


def pairings():
    size, groups = lax.axis_size("row"), lax.axis_size("grp")
    within = [(i, i ^ 1) for i in range(size)]
    between = []
    for g in range(groups):
        for i in range(size):
            j = i + 1 if i % 2 else i - 1
            if 0 <= j < size:
                target = g * size + j
            elif groups % 2 == 0:
                target = (g ^ 1) * size + i
            else:
                target = g * size + size - 1 - i
            between.append((g * size + i, target))
    return within, between


def across(outer):
    return lax.ppermute(outer, ("grp", "row"), pairings()[1])


def along(inner):
    return lax.ppermute(inner, "row", pairings()[0])


def row_sum(x):
    size = lax.axis_size("row")
    assert size & (size - 1) == 0
    step = 1
    while step < size:
        flips = [1] if step == 1 else [step + 1, 2 * step + 1, 3 * step] if 2 * step < size else [step + 1]
        x = functools.reduce(jnp.add, [x] + [lax.ppermute(x, "row", [(i, i ^ f) for i in range(size)]) for f in flips])
        step *= 1 + len(flips)
    return x


def program(diag_blocks, lower_coupling, upper_coupling, right_sides):
    rows, columns = right_sides.shape
    width = lower_coupling.shape[1]
    rim = pltpu.VMEM((width, columns), F32)
    panel = pltpu.VMEM((rows, columns), F32)
    sums_shape = pltpu.VMEM((SWEEPS, columns), F32)
    lanes = 128
    lower, upper = lower_coupling.T, upper_coupling.T
    outer = call(
        open_kernel,
        rim,
        diag_blocks, right_sides, lower, upper,
        hbm=(0, 1, 2, 3),
        scratch=[
            pltpu.VMEM((width, lanes), F32),
            pltpu.VMEM((width, columns), F32),
            pltpu.SemaphoreType.DMA((2,)),
        ],
    )
    message = across(outer)
    inner = call(inner_kernel, rim, diag_blocks, right_sides, free=(0, 1))
    inner = along(inner)
    half = pltpu.VMEM((rows // 2, columns), F32)
    all_terms = pltpu.VMEM((2 * rows, columns), BF16)
    coupling_shape = pltpu.VMEM((rows, 3 * width), BF16)
    diag, outward, inward, told, scale, x, terms, v, sums = call(
        setup_kernel,
        [
            pltpu.VMEM((rows, 2 * rows), BF16),
            coupling_shape,
            coupling_shape,
            pltpu.VMEM((8, width * width // 8), F32),
            pltpu.VMEM((rows, lanes), F32),
            panel,
            all_terms,
            half,
            sums_shape,
        ],
        diag_blocks, lower, upper, right_sides,
        free=(0, 1, 2, 3),
        flops=3 * rows * rows * columns,
    )
    known, heard = [], []
    halo_shape = pltpu.VMEM((3 * width, columns), BF16)
    for sweep in range(1, SWEEPS):
        if sweep < SWEEPS - 1:
            tell = [told] if sweep == 1 else []
            sent = call(
                send_kernel,
                pltpu.VMEM((width + 8 * len(tell), columns), F32),
                *tell, inner, x, v, inward, scale,
                flops=6 * width * width * columns,
            )
            ahead = across(sent)
        u = call(
            fill_kernel,
            panel,
            inner, terms, v, right_sides, diag, inward,
            free=(3,),
            flops=3 * rows * (rows + 2 * width) * columns,
        )
        if sweep == SWEEPS - 1:
            break
        halo, rim_values, *news = call(
            functools.partial(rim_kernel, sweep=sweep),
            [halo_shape, rim] + ([pltpu.VMEM((width, 3 * width), BF16)] if sweep == 2 else []),
            *known, message, x, u, outward, scale,
            flops=6 * width * width * columns,
        )
        inner = along(rim_values)
        heard = heard or news
        x, terms, v, kept, sums = call(
            functools.partial(sweep_kernel, sweep=sweep),
            [panel, all_terms, half, rim if heard else halo_shape, sums_shape],
            *heard, halo, x, terms, u, right_sides, diag, outward, scale, sums,
            free=(len(heard) + 4,),
            flops=3 * rows * (rows + 2 * width) * columns,
        )
        known, message = [kept], ahead
    halo, sums = call(
        functools.partial(last_kernel, sweep=SWEEPS - 1),
        [halo_shape, sums_shape],
        *known, message, u, outward, sums,
        flops=6 * rows * width * columns,
    )
    solution = call(close_kernel, jax.ShapeDtypeStruct((rows, columns), F32), halo, u, outward, x, scale, flops=10 * rows * columns)
    return solution, jnp.sqrt(row_sum(sums))


def solution(mesh):
    return jax.shard_map(
        program,
        mesh=mesh,
        in_specs=(P("row", None), P("row", None), P("row", None), P("row", "grp")),
        out_specs=(P("row", "grp"), P(None, "grp")),
        check_vma=False,
    )
```

```python
import functools

import jax
import jax.numpy as jnp
from jax import lax
from jax.experimental import pallas as pl
from jax.experimental.pallas import tpu as pltpu
from jax.sharding import PartitionSpec as P


SWEEPS = 8
F32 = jnp.float32
BF16 = jnp.bfloat16
VMEM_GRANT = 24 * 2**20
HBM_BLOCK = pl.BlockSpec(memory_space=pltpu.HBM)
VMEM_BLOCK = pl.BlockSpec(memory_space=pltpu.VMEM)


def call(kernel, outs, *args, hbm=(), free=(), scratch=(), flops=0):
    args = [a if i in free else pltpu.with_memory_space_constraint(a, pltpu.HBM if i in hbm else pltpu.VMEM) for i, a in enumerate(args)]
    many = isinstance(outs, list)
    return pl.pallas_call(
        kernel,
        out_shape=outs,
        in_specs=[HBM_BLOCK if i in hbm else VMEM_BLOCK for i in range(len(args))],
        out_specs=[VMEM_BLOCK] * len(outs) if many else VMEM_BLOCK,
        scratch_shapes=scratch,
        compiler_params=pltpu.CompilerParams(vmem_limit_bytes=VMEM_GRANT),
        cost_estimate=pl.CostEstimate(flops=flops, transcendentals=0, bytes_accessed=0),
    )(*args)


def halves(x):
    high = x.astype(BF16)
    return high, (x - high.astype(F32)).astype(BF16)


def left_terms(x):
    high, low = halves(x)
    return jnp.concatenate([high, low, high], axis=1)


def right_terms(x):
    high, low = halves(x)
    return jnp.concatenate([high, high, low], axis=0)


def both(x, axis):
    return jnp.concatenate(halves(x), axis=axis)


def product(left, right):
    return jnp.dot(left, right, preferred_element_type=F32)


def place():
    index, size = lax.axis_index("row"), lax.axis_size("row")
    return index % 2, jnp.logical_or(index == 0, index == size - 1)


def rims(rows, width):
    odd, _ = place()
    top = rows - width
    return pl.multiple_of(odd * top, width), pl.multiple_of((1 - odd) * top, width)


def diagonal(block, offset):
    row = lax.broadcasted_iota(jnp.int32, block.shape, 0) + offset
    column = lax.broadcasted_iota(jnp.int32, block.shape, 1)
    return jnp.sum(jnp.where(row == column, block, 0.0), axis=1, keepdims=True)


def facing(outer):
    _, end = place()
    return jnp.where(end, jnp.zeros_like(outer), outer)


def copies(pairs, sems):
    moves = [pltpu.make_async_copy(source, target, sems.at[i]) for i, (source, target) in enumerate(pairs)]
    for move in moves:
        move.start()
    return moves


def open_kernel(diag, sides, lower, upper, outer_out, corner, strip, sems):
    odd, _ = place()
    rows = sides.shape[0]
    width, lanes = corner.shape
    far, _ = rims(rows, width)
    tile = pl.ds(pl.multiple_of(odd * (rows - lanes), lanes), lanes)
    moves = copies([(diag.at[pl.ds(far, width), tile], corner), (sides.at[pl.ds(far, width)], strip)], sems)
    for move in moves:
        move.wait()
    outer_out[...] = facing(strip[...] / diagonal(corner[...], odd * (lanes - width)))


def inner_kernel(diag, sides, inner_out):
    odd, _ = place()
    rows = sides.shape[0]
    width, lanes = inner_out.shape[0], 128
    top = rows - width
    first = sides[:width, :] / diagonal(diag[:width, :lanes], 0)
    last = sides[top:, :] / diagonal(diag[top:, rows - lanes :], lanes - width)
    inner_out[...] = jnp.where(odd == 1, first, last)


def setup_kernel(block, low, up, sides, diag_out, outer_out, inner_out, told_out, scale_out, x_out, terms_out, v_out, sums_out):
    odd, _ = place()
    width, rows = low.shape
    side = sides[...]
    sums_out[0:1, :] = jnp.sum(side * side, axis=0, keepdims=True)
    scale = 1.0 / diagonal(block[...], 0)
    scale_out[...] = jnp.broadcast_to(scale, scale_out.shape)
    x = side * scale
    x_out[...] = x
    terms_out[...] = both(x, 0)
    early, late = spans(rows)
    cut = 2 * early.size
    diag_out[:cut, :] = both(block[early, :], 0)
    diag_out[cut:, :] = both(block[late, :], 0)
    v_out[...] = applied(sides, diag_out, terms_out, early, 0)
    low, up = low[...], up[...]
    outer = jnp.where(odd == 1, up, low).T
    outer_out[...] = left_terms(outer)
    told = jnp.where(odd == 1, outer[rows - width :], outer[:width])
    told = told * jnp.where(odd == 1, scale[rows - width :], scale[:width])
    told_out[...] = facing(packed(told))
    inner_out[...] = left_terms(jnp.where(odd == 1, low, up).T)


def packed(square):
    return jnp.concatenate([square[i : i + 8] for i in range(0, square.shape[0], 8)], axis=1)


def unpacked(strip, width):
    return jnp.concatenate([strip[:, i : i + width] for i in range(0, width * width // 8, width)], axis=0)


def early_rows(rows):
    return rows * 9 // 16


def spans(rows):
    odd, _ = place()
    early = early_rows(rows)
    late = rows - early
    tile = 32
    return pl.ds(pl.multiple_of(odd * late, tile), early), pl.ds(pl.multiple_of((1 - odd) * early, tile), late)


def applied(side, diag, terms, span, first):
    rows, some = side.shape[0], span.size
    images = product(diag[first : first + 2 * some, :], terms[:rows, :])
    images = images[:some] + images[some:] + product(diag[first : first + some, :], terms[rows:, :])
    return side[span, :] - images


def wide(pivots, columns):
    return jnp.concatenate([pivots] * (columns // pivots.shape[1]), axis=1)


def send_kernel(*refs):
    *told, inner, x, v, coupling, scale, outer_out = refs
    odd, _ = place()
    rows, columns = x.shape
    width = inner.shape[0]
    far, _ = rims(rows, width)
    rim = pl.ds(far, width)
    inside = pl.ds(pl.multiple_of(odd * (v.shape[0] - width), width), width)
    residual = v[inside, :] - product(coupling[rim, :], right_terms(inner[...]))
    outer_out[:width, :] = facing(x[rim, :] + residual * wide(scale[rim, :], columns))
    if told:
        outer_out[width:, :] = told[0][...]


def fill_kernel(inner, terms, v, side, diag, coupling, u_out):
    early, late = spans(side.shape[0])
    halo = right_terms(inner[...])
    u_out[early, :] = v[...] - product(coupling[early, :], halo)
    u_out[late, :] = applied(side, diag, terms, late, 2 * early.size) - product(coupling[late, :], halo)


def rim_kernel(*refs, sweep):
    told_out = None
    if sweep == 2:
        *refs, told_out = refs
    *known, message, x, u, coupling, scale, halo_out, inner_out = refs
    rows, columns = x.shape
    width = inner_out.shape[0]
    _, near = rims(rows, width)
    rim = pl.ds(near, width)
    outer = message[:width, :]
    if sweep == 2:
        told = left_terms(unpacked(message[width:, :], width))
        told_out[...] = told
        outer = outer - product(told, known[0][...])
    elif sweep > 2:
        outer = outer - known[0][...]
    halo = right_terms(outer)
    halo_out[...] = halo
    residual = u[rim, :] - product(coupling[rim, :], halo)
    inner_out[...] = x[rim, :] + residual * wide(scale[rim, :], columns)


def sweep_kernel(*refs, sweep):
    *told, halo, x, terms, u, side, diag, coupling, scale, sums, x_out, terms_out, v_out, known_out, sums_out = refs
    rows, columns = x.shape
    width = halo.shape[0] // 3
    far, _ = rims(rows, width)
    mine = jnp.concatenate([terms[pl.ds(far + part * rows, width), :] for part in (0, 0, 1)], axis=0)
    known_out[...] = product(told[0][...], mine) if told else mine
    sums_out[...] = sums[...]
    residual = u[...] - product(coupling[...], halo[...])
    sums_out[sweep : sweep + 1, :] = jnp.sum(residual * residual, axis=0, keepdims=True)
    new = x[...] + residual * wide(scale[...], columns)
    x_out[...] = new
    terms_out[...] = both(new, 0)
    early, _ = spans(rows)
    v_out[...] = applied(side, diag, terms_out, early, 0)


def last_kernel(known, message, u, coupling, sums, halo_out, sums_out, *, sweep):
    sums_out[...] = sums[...]
    halo = right_terms(message[...] - known[...])
    halo_out[...] = halo
    residual = u[...] - product(coupling[...], halo)
    sums_out[sweep : sweep + 1, :] = jnp.sum(residual * residual, axis=0, keepdims=True)


def close_kernel(halo, u, coupling, x, scale, x_out):
    residual = u[...] - product(coupling[...], halo[...])
    x_out[...] = x[...] + residual * wide(scale[...], x.shape[1])


def pairings():
    size, groups = lax.axis_size("row"), lax.axis_size("grp")
    within = [(i, i ^ 1) for i in range(size)]
    between = []
    for g in range(groups):
        for i in range(size):
            j = i + 1 if i % 2 else i - 1
            if 0 <= j < size:
                target = g * size + j
            elif groups % 2 == 0:
                target = (g ^ 1) * size + i
            else:
                target = g * size + size - 1 - i
            between.append((g * size + i, target))
    return within, between


def across(outer):
    return lax.ppermute(outer, ("grp", "row"), pairings()[1])


def along(inner):
    return lax.ppermute(inner, "row", pairings()[0])


def row_sum(x):
    size = lax.axis_size("row")
    assert size & (size - 1) == 0
    step = 1
    while step < size:
        flips = [1] if step == 1 else [step + 1, 2 * step + 1, 3 * step] if 2 * step < size else [step + 1]
        x = functools.reduce(jnp.add, [x] + [lax.ppermute(x, "row", [(i, i ^ f) for i in range(size)]) for f in flips])
        step *= 1 + len(flips)
    return x


def program(diag_blocks, lower_coupling, upper_coupling, right_sides):
    rows, columns = right_sides.shape
    width = lower_coupling.shape[1]
    rim = pltpu.VMEM((width, columns), F32)
    panel = pltpu.VMEM((rows, columns), F32)
    sums_shape = pltpu.VMEM((SWEEPS, columns), F32)
    lanes = 128
    lower, upper = lower_coupling.T, upper_coupling.T
    outer = call(
        open_kernel,
        rim,
        diag_blocks, right_sides, lower, upper,
        hbm=(0, 1, 2, 3),
        scratch=[
            pltpu.VMEM((width, lanes), F32),
            pltpu.VMEM((width, columns), F32),
            pltpu.SemaphoreType.DMA((2,)),
        ],
    )
    message = across(outer)
    inner = call(inner_kernel, rim, diag_blocks, right_sides, free=(0, 1))
    inner = along(inner)
    half = pltpu.VMEM((early_rows(rows), columns), F32)
    all_terms = pltpu.VMEM((2 * rows, columns), BF16)
    coupling_shape = pltpu.VMEM((rows, 3 * width), BF16)
    diag, outward, inward, told, scale, x, terms, v, sums = call(
        setup_kernel,
        [
            pltpu.VMEM((2 * rows, rows), BF16),
            coupling_shape,
            coupling_shape,
            pltpu.VMEM((8, width * width // 8), F32),
            pltpu.VMEM((rows, lanes), F32),
            panel,
            all_terms,
            half,
            sums_shape,
        ],
        diag_blocks, lower, upper, right_sides,
        free=(0, 1, 2, 3),
        flops=3 * rows * rows * columns,
    )
    known, heard = [], []
    halo_shape = pltpu.VMEM((3 * width, columns), BF16)
    for sweep in range(1, SWEEPS):
        if sweep < SWEEPS - 1:
            tell = [told] if sweep == 1 else []
            sent = call(
                send_kernel,
                pltpu.VMEM((width + 8 * len(tell), columns), F32),
                *tell, inner, x, v, inward, scale,
                flops=6 * width * width * columns,
            )
            ahead = across(sent)
        u = call(
            fill_kernel,
            panel,
            inner, terms, v, right_sides, diag, inward,
            free=(3,),
            flops=3 * rows * (rows + 2 * width) * columns,
        )
        if sweep == SWEEPS - 1:
            break
        halo, rim_values, *news = call(
            functools.partial(rim_kernel, sweep=sweep),
            [halo_shape, rim] + ([pltpu.VMEM((width, 3 * width), BF16)] if sweep == 2 else []),
            *known, message, x, u, outward, scale,
            flops=6 * width * width * columns,
        )
        inner = along(rim_values)
        heard = heard or news
        x, terms, v, kept, sums = call(
            functools.partial(sweep_kernel, sweep=sweep),
            [panel, all_terms, half, rim if heard else halo_shape, sums_shape],
            *heard, halo, x, terms, u, right_sides, diag, outward, scale, sums,
            free=(len(heard) + 4,),
            flops=3 * rows * (rows + 2 * width) * columns,
        )
        known, message = [kept], ahead
    halo, sums = call(
        functools.partial(last_kernel, sweep=SWEEPS - 1),
        [halo_shape, sums_shape],
        *known, message, u, outward, sums,
        flops=6 * rows * width * columns,
    )
    solution = call(close_kernel, jax.ShapeDtypeStruct((rows, columns), F32), halo, u, outward, x, scale, flops=10 * rows * columns)
    return solution, jnp.sqrt(row_sum(sums))


def solution(mesh):
    return jax.shard_map(
        program,
        mesh=mesh,
        in_specs=(P("row", None), P("row", None), P("row", None), P("row", "grp")),
        out_specs=(P("row", "grp"), P(None, "grp")),
        check_vma=False,
    )
```
